32 devices in a mesh: dp: 4 (over y, z), tp: 8 (over x, core).
Axes of the slice: x: 4, y: 2, z: 2, core: 2. Of those that a mesh axis runs over, the one named last changes fastest.
The devices are a block of a 4x4x8 slice.
Arguments:
- ids: int32 [8, 256], P('dp'), parts along dimension 0
- E: bfloat16 [32768, 2048], P('tp')
- g: bfloat16 [2048], replicated
- W: bfloat16 [2048, 3072], P(None, 'tp')
- du: bfloat16 [8, 256, 3072], P('dp', None, 'tp'), parts along dimension 0
- dres: bfloat16 [8, 256, 2048], P('dp', 'tp'), parts along dimension 0
Outputs:
- output 1: bfloat16 [8, 256, 3072], P('dp', None, 'tp'), parts along dimension 0
- output 2: bfloat16 [8, 256, 2048], P('dp', 'tp'), parts along dimension 0
- output 3: float32 [131072, 2048], P(('dp', 'tp')), parts along dimension 0
- output 4: float32 [8192, 3072], P('dp', 'tp'), parts along dimension 0
- output 5: float32 [8192], P('dp'), parts along dimension 0
There are 4 independent parts. The reference program is written for one: setup_inputs(seed, part) draws one part's arguments, and reference() takes and returns one part's arrays. A program takes and returns all parts, laid end to end along the dimension named above; an argument that names none is the same for every part.
All inputs are finite; a program needn't handle non-finite values.
Results may differ from the reference program's by a relative error of at most 0.00675624.
Values are sent between devices in bfloat16 or wider.
A program may use at most 768 MiB of HBM per device.

```python
import jax
import jax.numpy as jnp
from jax import lax

V = 32768
K = 2
T = 256
D = 2048
FC = 3072
TP = 8
NPOP = 256
EPS = 1e-6


def setup_inputs(seed: int = 0, part: int = 0) -> dict:
    key = jax.random.key(seed)
    kp = jax.random.fold_in(key, part)
    k1, k2, k3, k4, k5, k6 = jax.random.split(kp, 6)
    s1, s2, s3 = jax.random.split(key, 3)
    kd = jax.random.fold_in(kp, 7)
    d1, d2, d3, d4 = jax.random.split(kd, 4)
    vs = V // TP
    pop = jnp.arange(TP, dtype=jnp.int32) * vs + jax.random.randint(d1, (TP,), 0, vs, dtype=jnp.int32)
    pick = jax.random.randint(d2, (K, T), 0, TP, dtype=jnp.int32)
    uni = jax.random.randint(d3, (K, T), 0, V, dtype=jnp.int32)
    coin = jax.random.bernoulli(d4, 0.75, (K, T))
    ids = jnp.where(coin, pop[pick], uni).astype(jnp.int32)
    E = jax.random.normal(s1, (V, D), jnp.float32).astype(jnp.bfloat16)
    g = (1.0 + 0.4 * jax.random.normal(s2, (D,), jnp.float32)).astype(jnp.bfloat16)
    W = (jax.random.normal(s3, (D, FC), jnp.float32) * D ** -0.5).astype(jnp.bfloat16)
    du = jax.random.normal(k5, (K, T, FC), jnp.float32).astype(jnp.bfloat16)
    dres = jax.random.normal(k6, (K, T, D), jnp.float32).astype(jnp.bfloat16)
    return {"ids": ids, "E": E, "g": g, "W": W, "du": du, "dres": dres}


def reference(ids, E, g, W, du, dres):
    gf = g.astype(jnp.float32)
    fs = FC // TP
    wr = W.reshape(D, TP, fs).transpose(1, 0, 2)

    def micro(carry, inp):
        dE, dW, dg = carry
        idk, duk, dresk = inp
        x = jnp.take(E, idk, axis=0)
        xf = x.astype(jnp.float32)
        rs = lax.rsqrt(jnp.mean(xf * xf, axis=-1, keepdims=True) + EPS)
        nh = xf * rs
        n = (nh * gf).astype(jnp.bfloat16)
        u = jnp.dot(n, W, preferred_element_type=jnp.float32).astype(jnp.bfloat16)
        dur = duk.reshape(T, TP, fs).transpose(1, 0, 2)

        def add_block(acc, blk):
            dub, wb = blk
            pr = jnp.dot(dub, wb.T, preferred_element_type=jnp.float32)
            return acc + pr.astype(jnp.bfloat16).astype(jnp.float32), None

        dn, _ = lax.scan(add_block, jnp.zeros((T, D), jnp.float32), (dur, wr))
        gdn = gf * dn
        dx = dresk.astype(jnp.float32) + rs * (gdn - nh * jnp.mean(nh * gdn, axis=-1, keepdims=True))
        dxb = dx.astype(jnp.bfloat16).astype(jnp.float32)
        dE = dE.at[idk].add(dxb)
        dW = dW + jnp.dot(n.T, duk, preferred_element_type=jnp.float32)
        dg = dg + jnp.sum(dn * nh, axis=0)
        return (dE, dW, dg), (u, x)

    init = (jnp.zeros((V, D), jnp.float32), jnp.zeros((D, FC), jnp.float32), jnp.zeros((D,), jnp.float32))
    (dE, dW, dg), (u, x) = lax.scan(micro, init, (ids, du, dres))
    return u, x, dE, dW, dg
```

```python
import jax
import jax.numpy as jnp
from jax import lax
from jax.experimental import pallas as pl
from jax.experimental.pallas import tpu as pltpu
from jax.sharding import PartitionSpec as P

EPS = 1e-6
F32 = jnp.float32
BF16 = jnp.bfloat16
MESH = pl.DeviceIdType.MESH

PX, P1, P2, P3 = 0, 1, 3, 5
XX, X1, X2, X3 = 7, 8, 10, 12
AGX, AGD, DG, NSEM = 14, 28, 42, 49
A1, A2, A3, B0, B1, B2, B3 = 0, 2, 4, 6, 8, 10, 12


def comm_kernel(ids_ref, e_ref, g_ref, w_ref, du_ref, dres_ref,
                n_ref, dx_ref, x_ref, dg_ref,
                ev, acc, idc, p, pin, s, r1, fin, xp, xin, xr1, xfin, xfull, dxfull, dgall,
                esem, ssem, rsem):
    nk, ntp, ts, d = xfull.shape
    nchip = ntp // 2
    t = nk * ntp * ts
    ne, er, _ = ev.shape
    me = lax.axis_index("tp")
    c, k = me // 2, me % 2
    partner = 2 * c + 1 - k
    chips = [(c + 1) % nchip, (c + nchip - 1) % nchip]
    opp = (c + 2) % nchip
    nbr = [2 * q + k for q in chips]

    def rcopy(i, src, dst, to):
        return pltpu.make_async_remote_copy(
            src_ref=src, dst_ref=dst, send_sem=ssem.at[i], recv_sem=rsem.at[i],
            device_id={"tp": to}, device_id_type=MESH)

    def ecopy(i):
        return pltpu.make_async_copy(e_ref.at[i], ev.at[i], esem.at[i])

    barrier = pltpu.get_barrier_semaphore()
    for j in range(1, ntp):
        pl.semaphore_signal(barrier, inc=1, device_id={"tp": (me + j) % ntp}, device_id_type=MESH)
    for i in range(ne):
        ecopy(i).start()

    nt = 256

    @pl.loop(0, d // nt)
    def _(j):
        cols = pl.ds(pl.multiple_of(j * nt, nt), nt)
        o = lax.dot_general(du_ref[...], w_ref[cols, :], (((1,), (1,)), ((), ())),
                            preferred_element_type=F32).astype(BF16)
        p[:, :, :, :, cols] = o.reshape(nk, nchip, 2, ts, nt)

    pl.semaphore_wait(barrier, ntp - 1)
    cpx = rcopy(PX, p.at[:, :, 1 - k], pin, partner)
    cpx.start()

    for h in range(nk):
        row = jnp.broadcast_to(ids_ref[h:h + 1, :], (128, ntp * ts))
        idc[h * ntp * ts:(h + 1) * ntp * ts, :] = jnp.transpose(row)

    cpx.wait_recv()

    def pair(h, q):
        return p[h, q, k].astype(F32) + pin[h, q].astype(F32)

    sends = []
    for dr in range(2):
        s[dr, opp] = pair(dr, opp)
        cp = rcopy(P1 + dr, s.at[dr, opp], r1.at[dr], nbr[dr])
        cp.start()
        sends.append(cp)
    for dr in range(2):
        s[1 - dr, chips[dr]] = pair(1 - dr, chips[dr])
        cp = rcopy(P2 + dr, s.at[1 - dr, chips[dr]], fin.at[dr, 1 - dr], nbr[dr])
        cp.start()
        sends.append(cp)

    lo = me * (ne * er)
    lane = lax.broadcasted_iota(jnp.int32, (t, er), 1)
    acc[...] = jnp.zeros_like(acc)
    nc = 512

    @pl.loop(0, ne)
    def _(i):
        ecopy(i).wait()
        idv = idc[...] - (lo + i * er)
        oh = (jnp.concatenate([idv] * (er // 128), axis=1) == lane).astype(BF16)

        @pl.loop(0, d // nc)
        def _(j):
            cols = pl.ds(pl.multiple_of(j * nc, nc), nc)
            acc[:, cols] += jnp.dot(oh, ev[i, :, cols], preferred_element_type=F32)

    xp[...] = acc[...].astype(BF16).reshape(xp.shape)
    cxx = rcopy(XX, xp.at[:, :, 1 - k], xin, partner)
    cxx.start()
    cxx.wait_recv()

    def xpair(h, q):
        return (xp[h, q, k].astype(F32) + xin[h, q].astype(F32)).astype(BF16)

    cxx.wait_send()
    for dr in range(2):
        xp[dr, opp, k] = xpair(dr, opp)
        cp = rcopy(X1 + dr, xp.at[dr, opp, k], xr1.at[dr], nbr[dr])
        cp.start()
        sends.append(cp)
    for dr in range(2):
        xp[1 - dr, chips[dr], k] = xpair(1 - dr, chips[dr])
        cp = rcopy(X2 + dr, xp.at[1 - dr, chips[dr], k], xfin.at[dr, 1 - dr], nbr[dr])
        cp.start()
        sends.append(cp)
    for dr in range(2):
        v = xpair(dr, chips[dr]).astype(F32)
        rcopy(X1 + dr, xp.at[dr, opp, k], xr1.at[dr], nbr[dr]).wait_recv()
        xp[dr, chips[dr], k] = (v + xr1[dr].astype(F32)).astype(BF16)
        cp = rcopy(X3 + dr, xp.at[dr, chips[dr], k], xfin.at[dr, dr], nbr[dr])
        cp.start()
        sends.append(cp)
    for dr in range(2):
        rcopy(P1 + dr, s.at[dr, opp], r1.at[dr], nbr[dr]).wait_recv()
        s[dr, chips[dr]] = pair(dr, chips[dr]) + r1[dr]
        cp = rcopy(P3 + dr, s.at[dr, chips[dr]], fin.at[dr, dr], nbr[dr])
        cp.start()
        sends.append(cp)

    def ag_start(base, full):
        for dr in range(2):
            for m, h in ((A1, dr), (A2, 1 - dr)):
                cp = rcopy(base + m + dr, full.at[h, me], full.at[h, me], nbr[dr])
                cp.start()
                sends.append(cp)
        for h in range(2):
            cp = rcopy(base + B0 + h, full.at[h, me], full.at[h, me], partner)
            cp.start()
            sends.append(cp)

    def ag_recv(base, full, m, b, dr, h, owner, forward):
        blk = full.at[h, owner]
        rcopy(base + m + dr, blk, blk, nbr[dr]).wait_recv()
        if forward:
            cp = rcopy(base + A3 + dr, blk, blk, nbr[dr])
            cp.start()
            sends.append(cp)
        cp = rcopy(base + b + dr, blk, blk, partner)
        cp.start()
        sends.append(cp)

    def ag_near(base, full):
        for dr in range(2):
            ag_recv(base, full, A1, B1, dr, dr, nbr[1 - dr], True)
        for dr in range(2):
            ag_recv(base, full, A2, B2, dr, 1 - dr, nbr[1 - dr], False)

    def ag_far(base, full):
        for dr in range(2):
            ag_recv(base, full, A3, B3, dr, dr, 2 * opp + k, False)

    def ag_end(base, full):
        for b in (B0, B1, B2, B3):
            for i in range(2):
                blk = full.at[0, 0]
                rcopy(base + b + i, blk, blk, partner).wait_recv()

    for h in range(nk):
        v = xpair(h, c).astype(F32)
        for dr in range(2):
            m = X3 if h == dr else X2
            rcopy(m + dr, xfin.at[dr, h], xfin.at[dr, h], nbr[dr]).wait_recv()
            v = v + xfin[dr, h].astype(F32)
        v = v.astype(BF16)
        xfull[h, me] = v
        x_ref[h] = v
    ag_start(AGX, xfull)

    gf = g_ref[...].astype(F32)
    dgp = jnp.zeros((1, d), F32)
    for h in range(nk):
        xf = x_ref[h].astype(F32)
        rs = lax.rsqrt(jnp.mean(xf * xf, axis=-1, keepdims=True) + EPS)
        nh = xf * rs
        dn = pair(h, c)
        for dr in range(2):
            m = P3 if h == dr else P2
            rcopy(m + dr, fin.at[dr, h], fin.at[dr, h], nbr[dr]).wait_recv()
            dn = dn + fin[dr, h]
        gdn = gf * dn
        dxv = dres_ref[h].astype(F32) + rs * (gdn - nh * jnp.mean(nh * gdn, axis=-1, keepdims=True))
        dgp = dgp + jnp.sum(dn * nh, axis=0, keepdims=True)
        dxfull[h, me] = dxv.astype(BF16)
    ag_start(AGD, dxfull)
    dgall[me] = dgp
    for j in range(1, ntp):
        cp = rcopy(DG + j - 1, dgall.at[me], dgall.at[me], (me + j) % ntp)
        cp.start()
        sends.append(cp)

    ag_near(AGX, xfull)
    ag_near(AGD, dxfull)
    ag_far(AGX, xfull)
    ag_end(AGX, xfull)

    @pl.loop(0, nk * ntp)
    def _(i):
        h, q = i // ntp, i % ntp
        xf = xfull[h, q].astype(F32)
        rs = lax.rsqrt(jnp.mean(xf * xf, axis=-1, keepdims=True) + EPS)
        n_ref[h, q] = (xf * rs * gf).astype(BF16)

    for j in range(1, ntp):
        rcopy(DG + j - 1, dgall.at[me], dgall.at[me], (me + j) % ntp).wait_recv()
    tot = dgall[0]
    for j in range(1, ntp):
        tot = tot + dgall[j]
    dg_ref[...] = tot

    ag_far(AGD, dxfull)
    ag_end(AGD, dxfull)
    dx_ref[...] = dxfull[...]
    cpx.wait_send()
    for cp in sends:
        cp.wait_send()


def out_kernel(ids_ref, dx_ref, n_ref, nt_ref, du_ref, w_ref, x_ref, dg_ref,
               de_ref, dw_ref, u_ref, xo_ref, dgo_ref):
    i = pl.program_id(0)
    rows = de_ref.shape[0]
    nk, t = ids_ref.shape
    me = lax.axis_index("tp")
    lo = me * (rows * pl.num_programs(0)) + i * rows
    sub = lax.broadcasted_iota(jnp.int32, (rows, t), 0) + lo
    oh = jnp.concatenate([(ids_ref[h:h + 1, :] == sub).astype(BF16) for h in range(nk)], axis=1)
    de_ref[...] = jnp.dot(oh, dx_ref[...], preferred_element_type=F32)
    dw_ref[...] = lax.dot_general(nt_ref[...], du_ref[...], (((0,), (0,)), ((), ())),
                                  preferred_element_type=F32)

    @pl.when(i == 0)
    def _():
        xo_ref[...] = x_ref[...]
        dgo_ref[...] = dg_ref[...]

    @pl.when(i < nk)
    def _():
        r = pl.ds(pl.multiple_of(i * t, t), t)
        u_ref[...] = jnp.dot(n_ref[r, :], w_ref[...], preferred_element_type=F32).astype(BF16)


def solution(mesh):
    ntp = mesh.shape["tp"]

    def body(ids, E, g, W, du, dres):
        vs, d = E.shape
        nk, t = ids.shape
        ts = t // ntp
        fs = W.shape[1]
        nchip = ntp // 2
        er = 512
        ne = vs // er
        g2 = g.reshape(1, d)
        du2 = du.reshape(nk * t, fs)
        vm = pl.BlockSpec(memory_space=pltpu.VMEM)
        hb = pl.BlockSpec(memory_space=pl.ANY)
        n, dxa, x, dg = pl.pallas_call(
            comm_kernel,
            out_shape=(
                jax.ShapeDtypeStruct((nk, ntp, ts, d), BF16),
                jax.ShapeDtypeStruct((nk, ntp, ts, d), BF16),
                jax.ShapeDtypeStruct((nk, ts, d), BF16),
                jax.ShapeDtypeStruct((1, d), F32),
            ),
            in_specs=[vm, hb, vm, vm, vm, vm],
            out_specs=(vm, vm, vm, vm),
            scratch_shapes=[
                pltpu.VMEM((ne, er, d), BF16),
                pltpu.VMEM((nk * t, d), F32),
                pltpu.VMEM((nk * t, 128), jnp.int32),
                pltpu.VMEM((nk, nchip, 2, ts, d), BF16),
                pltpu.VMEM((nk, nchip, ts, d), BF16),
                pltpu.VMEM((nk, nchip, ts, d), F32),
                pltpu.VMEM((2, ts, d), F32),
                pltpu.VMEM((2, nk, ts, d), F32),
                pltpu.VMEM((nk, nchip, 2, ts, d), BF16),
                pltpu.VMEM((nk, nchip, ts, d), BF16),
                pltpu.VMEM((2, ts, d), BF16),
                pltpu.VMEM((2, nk, ts, d), BF16),
                pltpu.VMEM((nk, ntp, ts, d), BF16),
                pltpu.VMEM((nk, ntp, ts, d), BF16),
                pltpu.VMEM((ntp, 1, d), F32),
                pltpu.SemaphoreType.DMA((ne,)),
                pltpu.SemaphoreType.DMA((NSEM,)),
                pltpu.SemaphoreType.DMA((NSEM,)),
            ],
            compiler_params=pltpu.CompilerParams(
                collective_id=0, has_side_effects=True, vmem_limit_bytes=60 << 20),
            name="comm",
        )(ids, E.reshape(ne, er, d), g2, W, du2, dres)
        n2 = n.reshape(nk * t, d)
        rt = 256
        ng = vs // rt
        full = lambda *sh: pl.BlockSpec(sh, lambda i: (0,) * len(sh))
        dE, dW, u, xo, dgo = pl.pallas_call(
            out_kernel,
            grid=(ng,),
            out_shape=(
                jax.ShapeDtypeStruct((vs, d), F32),
                jax.ShapeDtypeStruct((d, fs), F32),
                jax.ShapeDtypeStruct((nk * t, fs), BF16),
                jax.ShapeDtypeStruct((nk, ts, d), BF16),
                jax.ShapeDtypeStruct((1, d), F32),
            ),
            in_specs=[
                full(nk, t), full(nk * t, d), full(nk * t, d),
                pl.BlockSpec((nk * t, d // ng), lambda i: (0, i)),
                full(nk * t, fs), full(d, fs), full(nk, ts, d), full(1, d),
            ],
            out_specs=(
                pl.BlockSpec((rt, d), lambda i: (i, 0)),
                pl.BlockSpec((d // ng, fs), lambda i: (i, 0)),
                pl.BlockSpec((t, fs), lambda i: (jnp.minimum(i, nk - 1), 0)),
                full(nk, ts, d), full(1, d),
            ),
            compiler_params=pltpu.CompilerParams(vmem_limit_bytes=48 << 20),
            name="outs",
        )(ids, dxa.reshape(nk * t, d), n2, n2, du2, W, x, dg)
        return u.reshape(nk, t, fs), xo, dE, dW, dgo.reshape(d)

    return jax.shard_map(
        body,
        mesh=mesh,
        in_specs=(P("dp", None), P("tp", None), P(None), P(None, "tp"), P("dp", None, "tp"), P("dp", "tp", None)),
        out_specs=(P("dp", None, "tp"), P("dp", "tp", None), P(("dp", "tp"), None), P("dp", "tp"), P("dp")),
        check_vma=False,
    )
```
